512 devices in a mesh: wide: 64 (over z_hi, y, core), narrow: 8 (over x, z_lo).
Axes of the slice: x: 4, y: 8, z: 8 (z_hi: 4, z_lo: 2; z = z_hi * 2 + z_lo), core: 2. Of those that a mesh axis runs over, the one named last changes fastest.
Arguments:
- enc_hidden: bfloat16 [12288, 6144], P('wide', 'narrow'), may hold values from -6 to 6
- enc_gain: float32 [6144], P('narrow'), may hold values from 0.1 to 1.9
- cross_weight: bfloat16 [6144, 256], P('narrow'), may hold values from -0.078125 to 0.078125
- assign: int32 [64], P('wide'), may hold values from 0 to 7
- token_ids: int32 [64, 2, 64], P('wide'), may hold values from 0 to 7999, as said below
- cross_table: bfloat16 [8000, 6144], P('wide', 'narrow'), may hold values from -540 to 540
- self_table: bfloat16 [8000, 6144], P('wide', 'narrow'), may hold values from -540 to 540
- kv_table: bfloat16 [8000, 256], P('wide'), may hold values from -6 to 6
- self_cache: bfloat16 [64, 64, 768, 256], P('wide', 'narrow'), may hold values from -6 to 6
Outputs:
- cross_out: bfloat16 [64, 2, 64, 6144], P('wide', None, None, 'narrow')
- self_out: bfloat16 [64, 2, 64, 6144], P('wide', None, 'narrow')
The draws below stay inside these ranges and needn't reach their ends.
Inputs may be any that keep to these rules, and one draw needn't show every extreme that they name: `token_ids`: within one group, at most 4 of its 128 ids lie in any one of the 64 ranges of 125 consecutive ids, and some range holds exactly 4 of them.
All inputs are finite; a program needn't handle non-finite values.
Results may differ from the reference program's by a relative error of at most 0.009.
The reference program's roundings to bfloat16 on the way count: a program that leaves them out, or rounds other values in their place, can miss the bound.
Values may be sent and summed in bfloat16 or wider, within the bound.
No kernel may reach another device: no remote copies, remote signals or barrier semaphores. Data moves between devices by JAX's collectives and lax.ppermute only.
A program may use at most 64 MiB of HBM per device.

```python
import jax
import jax.numpy as jnp
from jax import lax

D = 6144
HEADS = 48
HEAD = 128
VOCAB = 8000
STEPS = 2
ENC_LEN = 1536
CAND = 64
PREFIX = 768
PROBLEMS = 8
GROUPS = 64
ENC_ROWS = 12288
CAP = 4


def draw_token_ids(key, part):
    slots = GROUPS * CAP
    per_owner = VOCAB // GROUPS
    heavy = jax.random.randint(jax.random.fold_in(key, 11), (), 0, GROUPS)

    def one_group(group_key):
        order_key = jax.random.fold_in(group_key, 1)
        shuffle_key = jax.random.fold_in(group_key, 2)
        local_key = jax.random.fold_in(group_key, 3)
        order = jax.random.permutation(order_key, slots)
        owner = order // CAP
        score = jnp.where(owner == heavy, 0, 1) * slots + jnp.arange(slots)
        picked = jnp.argsort(score)[:STEPS * CAND]
        owners = jax.random.permutation(shuffle_key, owner[picked])
        local = jax.random.randint(local_key, (STEPS * CAND,), 0, per_owner)
        return (owners * per_owner + local).astype(jnp.int32).reshape(STEPS, CAND)
    group_keys = jax.random.split(jax.random.fold_in(key, 12), GROUPS)
    return jax.vmap(one_group)(group_keys)


def draw_cross_table(key, part):
    base = jnp.clip(jax.random.normal(jax.random.fold_in(key, 21), (VOCAB, HEADS * HEAD), jnp.float32), -6.0, 6.0) * 3.0
    return base.astype(jnp.bfloat16)


def draw_self_table(key, part):
    base = jnp.clip(jax.random.normal(jax.random.fold_in(key, 31), (VOCAB, HEADS * HEAD), jnp.float32), -6.0, 6.0) * 3.0
    return base.astype(jnp.bfloat16)


def plant(values, rng, low, top_value):
    shape = values.shape
    index_at = [jax.random.randint(jax.random.fold_in(rng, axis), (), 0, shape[axis]) for axis in range(len(shape))]
    values = values.at[tuple(index_at)].set(low)
    longest = shape.index(max(shape))
    index_at[longest] = (index_at[longest] + 1) % shape[longest]
    return values.at[tuple(index_at)].set(top_value)


def block_scale(own_key, shape, cuts, smallest, top_value):
    def one(dim, parts):
        draws = jax.random.uniform(jax.random.fold_in(jax.random.fold_in(own_key, 6), dim), (parts,), jnp.float32, smallest / len(cuts), top_value / len(cuts))
        return jnp.repeat(jnp.exp(draws), shape[dim] // parts).reshape((-1,) + (1,) * (len(shape) - dim - 1))

    level = one(*cuts[0])
    for cut in cuts[1:]:
        level = level * one(*cut)
    return level


def bell_draw(key, shape, scale, reach, shards=(), kind=jnp.bfloat16):
    entries = jax.random.normal(key, shape, jnp.float32) * scale
    if len(shards) > 0:
        entries = block_scale(key, shape, shards, -0.22, 0.18) * entries
    return jnp.clip(entries, min=-reach, max=reach).astype(kind)


def setup_inputs(seed: int = 0) -> dict:
    splits = jax.random.split(jax.random.key(seed), 10)
    enc_hidden = bell_draw(splits[0], (ENC_ROWS, D), 1.0, 6.0, ((0, 64), (1, 8)))
    enc_gain = jnp.clip(1.0 + 0.18 * jax.random.normal(splits[1], (D,), jnp.float32), 0.1, 1.9)
    cross_weight = bell_draw(splits[2], (D, 2 * HEAD), D ** -0.5, 0.078125, ((0, 8),))
    assign = plant(jax.random.randint(splits[3], (GROUPS,), 0, PROBLEMS), jax.random.fold_in(splits[3], 1), 0, PROBLEMS - 1).astype(jnp.int32)
    token_ids = draw_token_ids(jax.random.fold_in(splits[9], 71), 0)
    cross_table = draw_cross_table(jax.random.fold_in(splits[9], 71), 0)
    self_table = draw_self_table(jax.random.fold_in(splits[9], 71), 0)
    kv_table = bell_draw(splits[7], (VOCAB, 2 * HEAD), 1.0, 6.0, ((0, 64),))
    self_cache = bell_draw(splits[8], (GROUPS, CAND, PREFIX, 2 * HEAD), 1.0, 6.0, ((0, 64), (1, 8)))
    return dict(enc_hidden=enc_hidden, enc_gain=enc_gain, cross_weight=cross_weight, assign=assign, token_ids=token_ids, cross_table=cross_table, self_table=self_table, kv_table=kv_table, self_cache=self_cache)


EPS = 1e-06

def reference(enc_hidden, enc_gain, cross_weight, assign, token_ids, cross_table, self_table, kv_table, self_cache):
    hidden = enc_hidden.astype(jnp.float32)
    meansq = lax.optimization_barrier(jnp.mean(hidden * hidden, axis=1))
    scaled = (hidden * enc_gain.astype(jnp.float32)).astype(jnp.bfloat16)
    projected = jnp.dot(scaled, cross_weight, preferred_element_type=jnp.float32)
    enc_kv = (projected * lax.rsqrt(meansq + EPS)[:, None]).astype(jnp.bfloat16)
    enc_kv = enc_kv.reshape(PROBLEMS, ENC_LEN, 2 * HEAD)
    factor = HEAD ** (-0.5)

    def one_group(inputs):
        problem, ids, cache = inputs
        problem_kv = lax.dynamic_index_in_dim(enc_kv, problem.astype(jnp.int32), 0, keepdims=False)
        flat = ids.reshape(-1)
        cross_q = jnp.take(cross_table, flat, axis=0).astype(jnp.float32).reshape(STEPS * CAND, HEADS, HEAD)
        keys = problem_kv[:, :HEAD].astype(jnp.float32)
        values = problem_kv[:, HEAD:].astype(jnp.float32)
        scores = jnp.einsum('rhd,kd->rhk', cross_q, keys) * factor
        peak = lax.optimization_barrier(jnp.max(scores, axis=-1, keepdims=True))
        expo = jnp.exp(scores - peak)
        total = lax.optimization_barrier(jnp.sum(expo, axis=-1))
        weights = expo.astype(jnp.bfloat16).astype(jnp.float32)
        result = jnp.einsum('rhk,kd->rhd', weights, values) / total[..., None]
        cross = result.astype(jnp.bfloat16).reshape(STEPS, CAND, HEADS * HEAD)
        self_q = jnp.take(self_table, flat, axis=0).astype(jnp.float32).reshape(STEPS, CAND, HEADS, HEAD)
        new_kv = jnp.take(kv_table, flat, axis=0).reshape(STEPS, CAND, 2 * HEAD)
        all_kv = jnp.concatenate([cache, jnp.transpose(new_kv, (1, 0, 2))], axis=1).astype(jnp.float32)
        self_scores = jnp.einsum('tchd,cpd->tchp', self_q, all_kv[..., :HEAD]) * factor
        position = jnp.arange(PREFIX + STEPS, dtype=jnp.int32)
        step_index = jnp.arange(STEPS, dtype=jnp.int32)
        allowed = (position[None, :] < PREFIX + 1 + step_index[:, None])[:, None, None, :]
        masked = jnp.where(allowed, self_scores, -jnp.inf)
        self_peak = lax.optimization_barrier(jnp.max(masked, axis=-1, keepdims=True))
        self_expo = jnp.where(allowed, jnp.exp(masked - self_peak), 0.0)
        self_total = lax.optimization_barrier(jnp.sum(self_expo, axis=-1))
        self_weights = self_expo.astype(jnp.bfloat16).astype(jnp.float32)
        self_result = jnp.einsum('tchp,cpd->tchd', self_weights, all_kv[..., HEAD:]) / self_total[..., None]
        selfs = self_result.astype(jnp.bfloat16).reshape(STEPS, CAND, HEADS * HEAD)
        return (cross, selfs)
    cross_out, self_out = lax.map(one_group, (assign, token_ids, self_cache))
    return (cross_out, self_out)
```

```python
import jax
import jax.numpy as jnp
from jax import lax
from jax.experimental import pallas as pl
from jax.experimental.pallas import tpu as pltpu
from jax.sharding import Mesh
from jax.sharding import PartitionSpec as P

D = 6144
HEADS = 48
HEAD = 128
ENC_LEN = 1536
EPS = 1e-06
OWN = 125
PART = 8
CHUNK = 24
INTERPRET = False
F32 = jnp.float32
BF16 = jnp.bfloat16


def iota(shape, dim, dtype=F32):
    return lax.broadcasted_iota(jnp.int32, shape, dim).astype(dtype)


def call(kernel, outs, flops, **kw):
    return pl.pallas_call(
        kernel,
        out_shape=outs,
        interpret=INTERPRET,
        cost_estimate=pl.CostEstimate(flops=flops, bytes_accessed=1 << 20, transcendentals=0),
        **kw,
    )


def smem():
    return pl.BlockSpec(memory_space=pltpu.SMEM)


def vmem():
    return pl.BlockSpec(memory_space=pltpu.VMEM)


def onehot(hit):
    return jnp.where(hit, 1.0, 0.0).astype(BF16)


def pick(rows, table):
    return jnp.dot(rows, table, preferred_element_type=F32)


def request_kernel(assign_ref, ids_ref, req_ref, slot_ref):
    cand = ids_ref.shape[2]
    eye = iota((cand, cand), 0) == iota((cand, cand), 1)
    earlier = iota((cand, cand), 1) < iota((cand, cand), 0)
    lane = lax.broadcasted_iota(jnp.int32, (cand, 128), 1)
    lane_rank = jnp.where(lane < 8, lane & 3, 8).astype(F32)

    def column(row):
        return jnp.sum(jnp.where(eye, row, 0.0), axis=1, keepdims=True)

    total = jnp.zeros((64, 128), F32)
    own_rows = []
    for t in range(2):
        row = ids_ref[0, t : t + 1, :].astype(F32)
        own_row = jnp.floor((row + 0.5) * (1.0 / OWN))
        own = column(own_row)
        local = column(row) - own * OWN
        rank = jnp.sum(jnp.where(earlier & (own == own_row), 1.0, 0.0), axis=1, keepdims=True)
        for before in own_rows:
            rank = rank + jnp.sum(jnp.where(own == before, 1.0, 0.0), axis=1, keepdims=True)
        own_rows.append(own_row)
        slot_ref[t] = jnp.broadcast_to(own * 8.0 + rank, (cand, 128))
        left = onehot(iota((64, cand), 0) == own_row)
        right = jnp.where(rank == lane_rank, local + 1.0, 0.0)
        total = total + pick(left, right.astype(BF16))
    lane8 = lax.broadcasted_iota(jnp.int32, (64, 128), 1)
    asked = total - 1.0 + jnp.where((lane8 & 4) != 0, 128.0, 0.0)
    asked = jnp.where(total > 0.5, asked, -1.0)
    req_ref[...] = jnp.where(lane8 >= 64, assign_ref[0].astype(F32), asked)


def project_kernel(hidden_ref, gain_ref, weight_ref, out_ref):
    hidden = hidden_ref[...].astype(F32)
    scaled = (hidden * gain_ref[...]).astype(BF16)
    proj = jnp.dot(scaled, weight_ref[...], preferred_element_type=F32)
    squares = jnp.sum(hidden * hidden, axis=1, keepdims=True)
    lane = lax.broadcasted_iota(jnp.int32, (8, 256), 1)
    for k in range(PART):
        at = k * CHUNK
        out_ref[k, 0:CHUNK, :] = proj[at : at + CHUNK]
        tile = jnp.zeros((8, 256), F32)
        for m in range(CHUNK // 8):
            tile = jnp.where(lane == m, squares[at + 8 * m : at + 8 * m + 8], tile)
        out_ref[k, CHUNK : CHUNK + 8, :] = tile


def finish_kernel(arrived_ref, req_ref, out_ref):
    proj = arrived_ref[0, 0:CHUNK, :]
    squares = arrived_ref[0, CHUNK : CHUNK + 8, 0:128]
    for n in range(1, PART):
        proj = proj + arrived_ref[n, 0:CHUNK, :]
        squares = squares + arrived_ref[n, CHUNK : CHUNK + 8, 0:128]
    lane = lax.broadcasted_iota(jnp.int32, (8, 128), 1)
    row = lax.broadcasted_iota(jnp.int32, (8, 128), 0)
    parts = []
    for m in range(CHUNK // 8):
        total = jnp.sum(jnp.where(lane == m, squares, 0.0), axis=1, keepdims=True)
        parts.append(proj[8 * m : 8 * m + 8] * lax.rsqrt(total / D + EPS))
    whole = jnp.concatenate(parts, axis=0)
    for i in range(PART):
        three = whole[3 * i : 3 * i + 3]
        base = jnp.concatenate(
            [three[:, 0:HEAD], three[:, HEAD : 2 * HEAD], jnp.zeros((2, HEAD), F32)], axis=0
        )
        for p in range(PART):
            w = p * PART + i
            out_ref[w] = jnp.where(row == 6, req_ref[w : w + 1, :], base).astype(BF16)


def pack_kernel(place_ref, arrived_ref, cross_ref, self_ref, kv_ref, out_ref, table_ref, new_ref):
    outer = place_ref[0]
    rank = place_ref[2] >> 1
    table_ref[112:128, :] = jnp.zeros((16, table_ref.shape[1]), BF16)
    table_ref[240:256, :] = jnp.zeros((16, table_ref.shape[1]), BF16)
    new_ref[112:128, :] = jnp.zeros((16, HEAD), BF16)
    table_ref[0:OWN, :] = cross_ref[...]
    table_ref[128 : 128 + OWN, :] = self_ref[...]

    @pl.when((place_ref[2] & 1) == 0)
    def _():
        new_ref[0:OWN, :] = kv_ref[:, 0:HEAD]

    @pl.when((place_ref[2] & 1) == 1)
    def _():
        new_ref[0:OWN, :] = kv_ref[:, HEAD : 2 * HEAD]

    lane = lax.broadcasted_iota(jnp.int32, (64, 128), 1)
    j = lax.broadcasted_iota(jnp.int32, (64, 128), 0) & 7
    j_col = (lax.broadcasted_iota(jnp.int32, (64, 1), 0) & 7).astype(F32)
    want_extra = jnp.where(j == 6, rank, 64)
    outer_row = (outer * 8).astype(F32)
    lanes_table = iota((64, 256), 1)
    lanes_kv = iota((64, 512), 1)
    lanes_new = iota((64, 128), 1)
    for q in range(PART):
        at = 64 * q
        asked = arrived_ref[8 * q : 8 * q + 8].astype(F32)[:, 6:7, :]
        asked = jnp.broadcast_to(asked, (8, 8, 128)).reshape(64, 128)
        row = jnp.sum(jnp.where(lane == j, asked, 0.0), axis=1, keepdims=True)
        info = jnp.sum(jnp.where(lane == want_extra, asked, 0.0), axis=1, keepdims=True)
        own = jnp.where(j_col < 6.0, info * 64.0 + outer_row + j_col, -1.0)
        new = jnp.where(j_col == 6.0, info, -1.0)
        out_ref[at : at + 64, 0:768] = pick(onehot(lanes_table == row), table_ref[...]).astype(BF16)
        out_ref[at : at + 64, 768:896] = (
            pick(onehot(lanes_kv == own), arrived_ref[...].reshape(512, 128))
            + pick(onehot(lanes_new == new), new_ref[...])
        ).astype(BF16)


def unpack_kernel(place_ref, arrived_ref, slot_ref, cross_ref, out_ref):
    rank = (place_ref[2] >> 1).astype(F32)
    lanes = iota((128, 512), 1)
    spread = jnp.concatenate([slot_ref[0], slot_ref[1]], axis=0)[:, 0:1]
    cross_ref[...] = pick(onehot(lanes == spread), arrived_ref[:, 0:768]).astype(BF16)
    slot = jnp.concatenate(
        [slot_ref[t, 8 * k : 8 * k + 8] for k in range(PART) for t in range(2)], axis=0
    )[:, 0:1]
    self_q = pick(onehot(lanes == slot + 4.0), arrived_ref[:, 0:768]).astype(BF16)
    own_rank = slot - 8.0 * jnp.floor(slot * 0.125)
    piece = jnp.where(own_rank == rank, slot - own_rank + 6.0, -1.0)
    new = pick(onehot(lanes == piece), arrived_ref[:, 768:896]).astype(BF16)
    row = lax.broadcasted_iota(jnp.int32, (192, 512), 0)
    source = (row & 63) * 8 + (row >> 6)
    column = lax.broadcasted_iota(jnp.int32, (192, 512), 1)
    keys = pick(onehot(column == source), arrived_ref[:, 768:896]).astype(BF16)
    values = pick(onehot(column == source + 3), arrived_ref[:, 768:896]).astype(BF16)
    for k in range(PART):
        out_ref[k, :, 0:768] = self_q[16 * k : 16 * k + 16]
        out_ref[k, :, 768:896] = new[16 * k : 16 * k + 16]
        for m in range(12):
            at = 896 + 256 * m
            out_ref[k, :, at : at + 128] = keys[16 * m : 16 * m + 16]
            out_ref[k, :, at + 128 : at + 256] = values[16 * m : 16 * m + 16]


def exchange(
    enc_hidden, enc_gain, cross_weight, assign, token_ids, cross_table, self_table, kv_table
):
    place = jnp.stack([lax.axis_index("p"), lax.axis_index("i"), lax.axis_index("n")]).astype(
        jnp.int32
    )
    asked, slot = call(
        request_kernel,
        (jax.ShapeDtypeStruct((64, 128), F32), jax.ShapeDtypeStruct((2, 64, 128), F32)),
        1 << 20,
        in_specs=[smem(), vmem()],
        name="request",
    )(assign, token_ids)
    partial = call(
        project_kernel,
        jax.ShapeDtypeStruct((PART, CHUNK + 8, 256), F32),
        1 << 28,
        name="project",
    )(enc_hidden, enc_gain.reshape(1, -1), cross_weight)
    arrived = lax.all_to_all(partial, "n", 0, 0, tiled=True)
    finished = call(
        finish_kernel, jax.ShapeDtypeStruct((64, 8, 128), BF16), 1 << 20, name="finish"
    )(arrived, asked)
    arrived = lax.all_to_all(finished, ("p", "i"), 0, 0, tiled=True)
    packed = call(
        pack_kernel,
        jax.ShapeDtypeStruct((512, 896), BF16),
        1 << 28,
        in_specs=[smem(), vmem(), vmem(), vmem(), vmem()],
        scratch_shapes=[pltpu.VMEM((256, 768), BF16), pltpu.VMEM((128, 128), BF16)],
        name="pack",
    )(place, arrived, cross_table, self_table, kv_table)
    arrived = lax.all_to_all(packed.reshape(64, 8, 896), ("p", "i"), 0, 0, tiled=True)
    cross_q, message = call(
        unpack_kernel,
        (
            jax.ShapeDtypeStruct((128, 768), BF16),
            jax.ShapeDtypeStruct((PART, 16, 3968), BF16),
        ),
        1 << 28,
        in_specs=[smem(), vmem(), vmem()],
        name="unpack",
    )(place, arrived.reshape(512, 896), slot)
    arrived = lax.all_to_all(message, "n", 0, 0, tiled=True)
    return cross_q, arrived


def attend(cross_q, arrived, self_cache):
    factor = HEAD ** (-0.5)
    problem_kv = arrived[:, :, 896:].reshape(8, 16, 12, 256)
    problem_kv = jnp.transpose(problem_kv, (0, 2, 1, 3)).reshape(ENC_LEN, 256)
    keys = problem_kv[:, :HEAD]
    values = problem_kv[:, HEAD:]
    own_q = cross_q.reshape(128, 6, HEAD)
    scores = jnp.einsum("rhd,kd->rhk", own_q, keys, preferred_element_type=F32) * factor
    peak = jnp.max(scores, axis=-1, keepdims=True)
    expo = jnp.exp(scores - peak)
    total = jnp.sum(expo, axis=-1)
    result = (
        jnp.einsum("rhk,kd->rhd", expo.astype(BF16), values, preferred_element_type=F32)
        / total[..., None]
    )
    cross_out = result.astype(BF16).reshape(1, 2, 64, 768)

    queries = arrived[:, :, :768].reshape(8, 2, 8, 6, HEAD)
    queries = jnp.transpose(queries, (1, 2, 0, 3, 4)).reshape(2, 8, HEADS, HEAD)
    pieces = arrived[:, :, 768:896].astype(F32).reshape(4, 2, 2, 8, HEAD)
    fresh = jnp.sum(pieces, axis=0).astype(BF16)
    cache = self_cache[0]
    prefix_scores = (
        jnp.einsum("tchd,cpd->tchp", queries, cache[..., :HEAD], preferred_element_type=F32)
        * factor
    )
    fresh_scores = (
        jnp.einsum("tchd,jcd->tchj", queries, fresh[0], preferred_element_type=F32) * factor
    )
    step = jnp.arange(2, dtype=jnp.int32)
    allowed = (step[None, :] <= step[:, None])[:, None, None, :]
    fresh_masked = jnp.where(allowed, fresh_scores, -jnp.inf)
    peak = jnp.maximum(jnp.max(prefix_scores, axis=-1), jnp.max(fresh_masked, axis=-1))[..., None]
    prefix_expo = jnp.exp(prefix_scores - peak)
    fresh_expo = jnp.where(allowed, jnp.exp(fresh_masked - peak), 0.0)
    total = jnp.sum(prefix_expo, axis=-1) + jnp.sum(fresh_expo, axis=-1)
    summed = jnp.einsum(
        "tchp,cpd->tchd", prefix_expo.astype(BF16), cache[..., HEAD:], preferred_element_type=F32
    )
    summed = summed + jnp.einsum(
        "tchj,jcd->tchd", fresh_expo.astype(BF16), fresh[1], preferred_element_type=F32
    )
    self_out = (summed / total[..., None]).astype(BF16).reshape(1, 2, 8, HEADS * HEAD)
    return cross_out, self_out


def body(*args):
    cross_q, arrived = exchange(*args[:-1])
    return attend(cross_q, arrived, args[-1])


def specs():
    wide = ("p", "i")
    ins = (
        P(wide, "n"),
        P("n"),
        P("n", None),
        P(wide),
        P(wide, None, None),
        P(wide, "n"),
        P(wide, "n"),
        P(wide, None),
        P(wide, "n", None, None),
    )
    return ins, (P(wide, None, None, "n"), P(wide, None, "n", None))


def solution(mesh):
    cut = Mesh(mesh.devices.reshape(PART, PART, PART), ("p", "i", "n"))
    ins, outs = specs()
    return jax.shard_map(body, mesh=cut, in_specs=ins, out_specs=outs, check_vma=False)
```

```python
import jax
import jax.numpy as jnp
from jax import lax
from jax.experimental import pallas as pl
from jax.experimental.pallas import tpu as pltpu
from jax.sharding import Mesh
from jax.sharding import PartitionSpec as P

D = 6144
HEADS = 48
HEAD = 128
EPS = 1e-06
OWN = 125
PART = 8
CHUNK = 24
LOG2E = 1.4426950408889634
INTERPRET = False
F32 = jnp.float32
BF16 = jnp.bfloat16


def iota(shape, dim, dtype=F32):
    return lax.broadcasted_iota(jnp.int32, shape, dim).astype(dtype)


def call(kernel, outs, flops, **kw):
    return pl.pallas_call(
        kernel,
        out_shape=outs,
        interpret=INTERPRET,
        cost_estimate=pl.CostEstimate(flops=flops, bytes_accessed=1 << 20, transcendentals=0),
        **kw,
    )


def smem():
    return pl.BlockSpec(memory_space=pltpu.SMEM)


def vmem():
    return pl.BlockSpec(memory_space=pltpu.VMEM)


def anywhere():
    return pl.BlockSpec(memory_space=pl.ANY)


def held(x):
    return pltpu.with_memory_space_constraint(x, pltpu.VMEM)


def onehot(hit):
    return jnp.where(hit, 1.0, 0.0).astype(BF16)


def pick(rows, table):
    return jnp.dot(rows, table, preferred_element_type=F32)


def request(assign_ref, ids_ref, req_ref, slot_ref):
    cand = ids_ref.shape[2]
    eye = iota((cand, cand), 0) == iota((cand, cand), 1)
    earlier = iota((cand, cand), 1) < iota((cand, cand), 0)
    lane = lax.broadcasted_iota(jnp.int32, (cand, 128), 1)
    lane_rank = jnp.where(lane < 8, lane & 3, 8).astype(F32)

    def column(row):
        return jnp.sum(jnp.where(eye, row, 0.0), axis=1, keepdims=True)

    total = jnp.zeros((64, 128), F32)
    own_rows = []
    for t in range(2):
        row = ids_ref[0, t : t + 1, :].astype(F32)
        own_row = jnp.floor((row + 0.5) * (1.0 / OWN))
        own = column(own_row)
        local = column(row) - own * OWN
        rank = jnp.sum(jnp.where(earlier & (own == own_row), 1.0, 0.0), axis=1, keepdims=True)
        for before in own_rows:
            rank = rank + jnp.sum(jnp.where(own == before, 1.0, 0.0), axis=1, keepdims=True)
        own_rows.append(own_row)
        slot_ref[t] = jnp.broadcast_to(own * 8.0 + rank, (cand, 128))
        left = onehot(iota((64, cand), 0) == own_row)
        right = jnp.where(rank == lane_rank, local + 1.0, 0.0)
        total = total + pick(left, right.astype(BF16))
    lane8 = lax.broadcasted_iota(jnp.int32, (64, 128), 1)
    asked = total - 1.0 + jnp.where((lane8 & 4) != 0, 128.0, 0.0)
    asked = jnp.where(total > 0.5, asked, -1.0)
    req_ref[...] = jnp.where(lane8 >= 64, assign_ref[0].astype(F32), asked)


def project_kernel(assign_ref, ids_ref, hidden_ref, gain_ref, weight_ref, *refs):
    req_ref, slot_ref, out_ref = refs[3:6]
    copies = [pltpu.make_async_copy(refs[k], refs[6 + k], refs[9].at[k]) for k in range(3)]
    for copy in copies:
        copy.start()
    hidden = hidden_ref[...].astype(F32)
    scaled = (hidden * gain_ref[...].reshape(1, -1)).astype(BF16)
    proj = jnp.dot(scaled, weight_ref[...], preferred_element_type=F32)
    squares = jnp.sum(hidden * hidden, axis=1, keepdims=True)
    lane = lax.broadcasted_iota(jnp.int32, (8, 256), 1)
    for k in range(PART):
        at = k * CHUNK
        out_ref[k, 0:CHUNK, :] = proj[at : at + CHUNK]
        tile = jnp.zeros((8, 256), F32)
        for m in range(CHUNK // 8):
            tile = jnp.where(lane == m, squares[at + 8 * m : at + 8 * m + 8], tile)
        out_ref[k, CHUNK : CHUNK + 8, :] = tile
    request(assign_ref, ids_ref, req_ref, slot_ref)
    for copy in copies:
        copy.wait()


def finish_kernel(arrived_ref, req_ref, out_ref):
    proj = arrived_ref[0, 0:CHUNK, :]
    squares = arrived_ref[0, CHUNK : CHUNK + 8, 0:128]
    for n in range(1, PART):
        proj = proj + arrived_ref[n, 0:CHUNK, :]
        squares = squares + arrived_ref[n, CHUNK : CHUNK + 8, 0:128]
    lane = lax.broadcasted_iota(jnp.int32, (8, 128), 1)
    row = lax.broadcasted_iota(jnp.int32, (8, 128), 0)
    parts = []
    for m in range(CHUNK // 8):
        total = jnp.sum(jnp.where(lane == m, squares, 0.0), axis=1, keepdims=True)
        parts.append(proj[8 * m : 8 * m + 8] * lax.rsqrt(total / D + EPS))
    whole = jnp.concatenate(parts, axis=0)
    for i in range(PART):
        three = whole[3 * i : 3 * i + 3]
        base = jnp.concatenate(
            [three[:, 0:HEAD], three[:, HEAD : 2 * HEAD], jnp.zeros((2, HEAD), F32)], axis=0
        )
        for p in range(PART):
            w = p * PART + i
            out_ref[w] = jnp.where(row == 6, req_ref[w : w + 1, :], base).astype(BF16)


def pack_kernel(arrived_ref, cross_ref, self_ref, kv_ref, out_ref, table_ref, new_ref):
    outer = lax.axis_index("p")
    narrow = lax.axis_index("n")
    rank = narrow >> 1
    table_ref[112:128, :] = jnp.zeros((16, table_ref.shape[1]), BF16)
    table_ref[240:256, :] = jnp.zeros((16, table_ref.shape[1]), BF16)
    new_ref[112:128, :] = jnp.zeros((16, HEAD), BF16)
    table_ref[0:OWN, :] = cross_ref[...]
    table_ref[128 : 128 + OWN, :] = self_ref[...]

    @pl.when((narrow & 1) == 0)
    def _():
        new_ref[0:OWN, :] = kv_ref[:, 0:HEAD]

    @pl.when((narrow & 1) == 1)
    def _():
        new_ref[0:OWN, :] = kv_ref[:, HEAD : 2 * HEAD]

    lane = lax.broadcasted_iota(jnp.int32, (64, 128), 1)
    j = lax.broadcasted_iota(jnp.int32, (64, 128), 0) & 7
    j_col = (lax.broadcasted_iota(jnp.int32, (64, 1), 0) & 7).astype(F32)
    want_extra = jnp.where(j == 6, rank, 64)
    outer_row = (outer * 8).astype(F32)
    lanes_table = iota((64, 256), 1)
    lanes_kv = iota((64, 512), 1)
    lanes_new = iota((64, 128), 1)
    for q in range(PART):
        at = 64 * q
        asked = arrived_ref[8 * q : 8 * q + 8].astype(F32)[:, 6:7, :]
        asked = jnp.broadcast_to(asked, (8, 8, 128)).reshape(64, 128)
        row = jnp.sum(jnp.where(lane == j, asked, 0.0), axis=1, keepdims=True)
        info = jnp.sum(jnp.where(lane == want_extra, asked, 0.0), axis=1, keepdims=True)
        own = jnp.where(j_col < 6.0, info * 64.0 + outer_row + j_col, -1.0)
        new = jnp.where(j_col == 6.0, info, -1.0)
        out_ref[at : at + 64, 0:768] = pick(onehot(lanes_table == row), table_ref[...]).astype(BF16)
        out_ref[at : at + 64, 768:896] = (
            pick(onehot(lanes_kv == own), arrived_ref[...].reshape(512, 128))
            + pick(onehot(lanes_new == new), new_ref[...])
        ).astype(BF16)


def unpack_kernel(arrived_ref, slot_ref, cross_ref, out_ref):
    rank = (lax.axis_index("n") >> 1).astype(F32)
    lanes = iota((128, 512), 1)
    spread = jnp.concatenate([slot_ref[0], slot_ref[1]], axis=0)[:, 0:1]
    cross_ref[...] = pick(onehot(lanes == spread), arrived_ref[:, 0:768]).astype(BF16)
    slot = jnp.concatenate(
        [slot_ref[t, 8 * k : 8 * k + 8] for k in range(PART) for t in range(2)], axis=0
    )[:, 0:1]
    self_q = pick(onehot(lanes == slot + 4.0), arrived_ref[:, 0:768]).astype(BF16)
    own_rank = slot - 8.0 * jnp.floor(slot * 0.125)
    piece = jnp.where(own_rank == rank, slot - own_rank + 6.0, -1.0)
    new = pick(onehot(lanes == piece), arrived_ref[:, 768:896]).astype(BF16)
    row = lax.broadcasted_iota(jnp.int32, (192, 512), 0)
    source = (row & 63) * 8 + (row >> 6)
    column = lax.broadcasted_iota(jnp.int32, (192, 512), 1)
    keys = pick(onehot(column == source), arrived_ref[:, 768:896]).astype(BF16)
    values = pick(onehot(column == source + 3), arrived_ref[:, 768:896]).astype(BF16)
    for k in range(PART):
        out_ref[k, :, 0:768] = self_q[16 * k : 16 * k + 16]
        out_ref[k, :, 768:896] = new[16 * k : 16 * k + 16]
        for m in range(12):
            at = 896 + 256 * m
            out_ref[k, :, at : at + 128] = keys[16 * m : 16 * m + 16]
            out_ref[k, :, at + 128 : at + 256] = values[16 * m : 16 * m + 16]


def exchange(
    enc_hidden, enc_gain, cross_weight, assign, token_ids, cross_table, self_table, kv_table
):
    tables = (cross_table, self_table, kv_table)
    asked, slot, partial, *tables = call(
        project_kernel,
        (
            pltpu.VMEM((64, 128), F32),
            pltpu.VMEM((2, 64, 128), F32),
            pltpu.VMEM((PART, CHUNK + 8, 256), F32),
            *[pltpu.VMEM(x.shape, x.dtype) for x in tables],
        ),
        1 << 28,
        in_specs=[smem(), vmem(), vmem(), vmem(), vmem(), anywhere(), anywhere(), anywhere()],
        scratch_shapes=[pltpu.SemaphoreType.DMA((3,))],
        name="project",
    )(assign, token_ids, enc_hidden, enc_gain, cross_weight, *tables)
    arrived = lax.all_to_all(partial, "n", 0, 0, tiled=True)
    finished = call(finish_kernel, pltpu.VMEM((64, 8, 128), BF16), 1 << 20, name="finish")(
        held(arrived), held(asked)
    )
    arrived = lax.all_to_all(finished, ("p", "i"), 0, 0, tiled=True)
    packed = call(
        pack_kernel,
        pltpu.VMEM((512, 896), BF16),
        1 << 28,
        scratch_shapes=[pltpu.VMEM((256, 768), BF16), pltpu.VMEM((128, 128), BF16)],
        name="pack",
    )(held(arrived), *[held(x) for x in tables])
    arrived = lax.all_to_all(packed.reshape(64, 8, 896), ("p", "i"), 0, 0, tiled=True)
    cross_q, message = call(
        unpack_kernel,
        (pltpu.VMEM((128, 768), BF16), pltpu.VMEM((PART, 16, 3968), BF16)),
        1 << 28,
        name="unpack",
    )(held(arrived.reshape(512, 896)), held(slot))
    arrived = lax.all_to_all(message, "n", 0, 0, tiled=True)
    return cross_q, arrived


def attend_kernel(
    query_ref,
    arrived_ref,
    far_cache_ref,
    cross_ref,
    self_ref,
    stack_ref,
    key_ref,
    value_ref,
    own_ref,
    result_ref,
    cache_ref,
    arrival,
):
    fetch = pltpu.make_async_copy(far_cache_ref, cache_ref, arrival)
    fetch.start()
    scale = LOG2E * HEAD ** (-0.5)
    across = (((1,), (1,)), ((), ()))

    for n in range(PART):
        for m in range(12):
            at, lane = 192 * n + 16 * m, 896 + 256 * m
            key_ref[at : at + 16, :] = arrived_ref[n, :, lane : lane + HEAD]
            value_ref[at : at + 16, :] = arrived_ref[n, :, lane + HEAD : lane + 2 * HEAD]
    for h in range(6):
        stack_ref[128 * h : 128 * h + 128, :] = query_ref[:, h * HEAD : (h + 1) * HEAD]

    for b in range(2):
        query = stack_ref[384 * b : 384 * b + 384, :]
        scores = [
            lax.dot_general(
                query, key_ref[512 * k : 512 * k + 512, :], across, preferred_element_type=F32
            )
            for k in range(3)
        ]
        peak = jnp.max(scores[0], axis=1, keepdims=True)
        for s in scores[1:]:
            peak = jnp.maximum(peak, jnp.max(s, axis=1, keepdims=True))
        total = jnp.zeros((384, 1), F32)
        result = jnp.zeros((384, HEAD), F32)
        for k in range(3):
            expo = jnp.exp2((scores[k] - peak) * scale)
            total = total + jnp.sum(expo, axis=1, keepdims=True)
            result = result + pick(expo.astype(BF16), value_ref[512 * k : 512 * k + 512, :])
        result = (result / total).astype(BF16)
        for h in range(3):
            at = (3 * b + h) * HEAD
            cross_ref[:, at : at + HEAD] = result[128 * h : 128 * h + 128]

    new_key = arrived_ref[0, :, 768:896].astype(F32)
    new_value = arrived_ref[1, :, 768:896].astype(F32)
    for n in range(2, PART, 2):
        new_key = new_key + arrived_ref[n, :, 768:896].astype(F32)
        new_value = new_value + arrived_ref[n + 1, :, 768:896].astype(F32)
    for n in range(PART):
        for h in range(6):
            tile = arrived_ref[n, :, h * HEAD : (h + 1) * HEAD].astype(F32)
            for t in range(2):
                at = 8 * (48 * t + 6 * n + h)
                own_ref[at : at + 8, :] = tile[8 * t : 8 * t + 8]

    fetch.wait()
    second = lax.broadcasted_iota(jnp.int32, (96, 1), 0) >= 48
    for c in range(8):
        query = own_ref[pl.ds(c, 96, stride=8), :]
        scores = lax.dot_general(
            query.astype(BF16), cache_ref[c, :, 0:HEAD], across, preferred_element_type=F32
        )
        fresh = [
            jnp.sum(query * new_key[8 * j + c : 8 * j + c + 1], axis=1, keepdims=True)
            for j in range(2)
        ]
        fresh[1] = jnp.where(second, fresh[1], -jnp.inf)
        peak = jnp.max(scores, axis=1, keepdims=True)
        peak = jnp.maximum(peak, jnp.maximum(fresh[0], fresh[1]))
        expo = jnp.exp2((scores - peak) * scale)
        total = jnp.sum(expo, axis=1, keepdims=True)
        result = pick(expo.astype(BF16), cache_ref[c, :, HEAD : 2 * HEAD])
        for j in range(2):
            weight = jnp.exp2((fresh[j] - peak) * scale)
            total = total + weight
            rounded = weight.astype(BF16).astype(F32)
            result = result + rounded * new_value[8 * j + c : 8 * j + c + 1]
        result_ref[pl.ds(c, 96, stride=8), :] = result / total

    for t in range(2):
        for h in range(HEADS):
            at = 8 * (HEADS * t + h)
            self_ref[t, :, h * HEAD : (h + 1) * HEAD] = result_ref[at : at + 8, :].astype(BF16)


def attend(cross_q, arrived, self_cache):
    cross_out, self_out = call(
        attend_kernel,
        (
            jax.ShapeDtypeStruct((128, 768), BF16),
            jax.ShapeDtypeStruct((2, 8, HEADS * HEAD), BF16),
        ),
        1 << 30,
        scratch_shapes=[
            pltpu.VMEM((768, HEAD), BF16),
            pltpu.VMEM((1536, HEAD), BF16),
            pltpu.VMEM((1536, HEAD), BF16),
            pltpu.VMEM((768, HEAD), F32),
            pltpu.VMEM((768, HEAD), F32),
            pltpu.VMEM(self_cache.shape[1:], BF16),
            pltpu.SemaphoreType.DMA,
        ],
        in_specs=[vmem(), vmem(), anywhere()],
        name="attend",
    )(held(cross_q), held(arrived), self_cache[0])
    return cross_out.reshape(1, 2, 64, 768), self_out[None]


def body(*args):
    cross_q, arrived = exchange(*args[:-1])
    return attend(cross_q, arrived, args[-1])


def specs():
    wide = ("p", "i")
    ins = (
        P(wide, "n"),
        P("n"),
        P("n", None),
        P(wide),
        P(wide, None, None),
        P(wide, "n"),
        P(wide, "n"),
        P(wide, None),
        P(wide, "n", None, None),
    )
    return ins, (P(wide, None, None, "n"), P(wide, None, "n", None))


def solution(mesh):
    cut = Mesh(mesh.devices.reshape(PART, PART, PART), ("p", "i", "n"))
    ins, outs = specs()
    return jax.shard_map(body, mesh=cut, in_specs=ins, out_specs=outs, check_vma=False)
```

```python
import jax
import jax.numpy as jnp
from jax import lax
from jax.experimental import pallas as pl
from jax.experimental.pallas import tpu as pltpu
from jax.sharding import Mesh
from jax.sharding import PartitionSpec as P

D = 6144
HEADS = 48
HEAD = 128
EPS = 1e-06
OWN = 125
PART = 8
CHUNK = 24
LOG2E = 1.4426950408889634
INTERPRET = False
F32 = jnp.float32
BF16 = jnp.bfloat16


def iota(shape, dim, dtype=F32):
    return lax.broadcasted_iota(jnp.int32, shape, dim).astype(dtype)


def call(kernel, outs, flops, **kw):
    return pl.pallas_call(
        kernel,
        out_shape=outs,
        interpret=INTERPRET,
        cost_estimate=pl.CostEstimate(flops=flops, bytes_accessed=1 << 20, transcendentals=0),
        **kw,
    )


def smem():
    return pl.BlockSpec(memory_space=pltpu.SMEM)


def vmem():
    return pl.BlockSpec(memory_space=pltpu.VMEM)


def anywhere():
    return pl.BlockSpec(memory_space=pl.ANY)


def held(x):
    return pltpu.with_memory_space_constraint(x, pltpu.VMEM)


def onehot(hit):
    return jnp.where(hit, 1.0, 0.0).astype(BF16)


def pick(rows, table):
    return jnp.dot(rows, table, preferred_element_type=F32)


def request(assign_ref, ids_ref, req_ref, slot_ref):
    cand = ids_ref.shape[2]
    eye = iota((cand, cand), 0) == iota((cand, cand), 1)
    earlier = iota((cand, cand), 1) < iota((cand, cand), 0)
    lane = lax.broadcasted_iota(jnp.int32, (cand, 128), 1)
    lane_rank = jnp.where(lane < 8, lane & 3, 8).astype(F32)

    def column(row):
        return jnp.sum(jnp.where(eye, row, 0.0), axis=1, keepdims=True)

    total = jnp.zeros((64, 128), F32)
    own_rows = []
    for t in range(2):
        row = ids_ref[0, t : t + 1, :].astype(F32)
        own_row = jnp.floor((row + 0.5) * (1.0 / OWN))
        own = column(own_row)
        local = column(row) - own * OWN
        rank = jnp.sum(jnp.where(earlier & (own == own_row), 1.0, 0.0), axis=1, keepdims=True)
        for before in own_rows:
            rank = rank + jnp.sum(jnp.where(own == before, 1.0, 0.0), axis=1, keepdims=True)
        own_rows.append(own_row)
        slot_ref[t] = jnp.broadcast_to(own * 8.0 + rank, (cand, 128))
        left = onehot(iota((64, cand), 0) == own_row)
        right = jnp.where(rank == lane_rank, local + 1.0, 0.0)
        total = total + pick(left, right.astype(BF16))
    lane8 = lax.broadcasted_iota(jnp.int32, (64, 128), 1)
    asked = total - 1.0 + jnp.where((lane8 & 4) != 0, 128.0, 0.0)
    asked = jnp.where(total > 0.5, asked, -1.0)
    problem = assign_ref[...].astype(F32).reshape(1, 1)
    req_ref[...] = jnp.where(lane8 >= 64, problem, asked)


def project_kernel(assign_ref, ids_ref, gain_ref, far_hidden_ref, far_weight_ref, *refs):
    req_ref, slot_ref, out_ref = refs[3:6]
    far = (far_hidden_ref, far_weight_ref, *refs[0:3])
    hidden_ref, weight_ref = refs[9:11]
    near = (hidden_ref, weight_ref, *refs[6:9])
    copies = [pltpu.make_async_copy(far[k], near[k], refs[11].at[k]) for k in range(5)]
    for copy in copies:
        copy.start()
    copies[0].wait()
    hidden = hidden_ref[...].astype(F32)
    scaled = (hidden * gain_ref[...].reshape(1, -1)).astype(BF16)
    copies[1].wait()
    proj = jnp.dot(scaled, weight_ref[...], preferred_element_type=F32)
    squares = jnp.sum(hidden * hidden, axis=1, keepdims=True)
    lane = lax.broadcasted_iota(jnp.int32, (8, 128), 1)
    for k in range(PART):
        tile = jnp.zeros((8, 128), F32)
        for m in range(CHUNK // 8):
            at = k * CHUNK + 8 * m
            out_ref[k, :, 256 * m : 256 * m + 256] = proj[at : at + 8]
            tile = jnp.where(lane == m, squares[at : at + 8], tile)
        out_ref[k, :, 768:896] = tile
    request(assign_ref, ids_ref, req_ref, slot_ref)
    for copy in copies[2:]:
        copy.wait()


def finish_kernel(arrived_ref, req_ref, out_ref):
    message = arrived_ref[0]
    for n in range(1, PART):
        message = message + arrived_ref[n]
    lane = lax.broadcasted_iota(jnp.int32, (8, 128), 1)
    row = lax.broadcasted_iota(jnp.int32, (8, 128), 0)
    parts = []
    for m in range(CHUNK // 8):
        total = jnp.sum(jnp.where(lane == m, message[:, 768:896], 0.0), axis=1, keepdims=True)
        parts.append(message[:, 256 * m : 256 * m + 256] * lax.rsqrt(total / D + EPS))
    whole = jnp.concatenate(parts, axis=0)
    for i in range(PART):
        three = whole[3 * i : 3 * i + 3]
        base = jnp.concatenate(
            [three[:, 0:HEAD], three[:, HEAD : 2 * HEAD], jnp.zeros((2, HEAD), F32)], axis=0
        )
        for p in range(PART):
            w = p * PART + i
            out_ref[w] = jnp.where(row == 6, req_ref[w : w + 1, :], base).astype(BF16)


def pack_kernel(arrived_ref, cross_ref, self_ref, kv_ref, out_ref, table_ref, new_ref):
    outer = lax.axis_index("p")
    narrow = lax.axis_index("n")
    rank = narrow >> 1
    table_ref[112:128, :] = jnp.zeros((16, table_ref.shape[1]), BF16)
    table_ref[240:256, :] = jnp.zeros((16, table_ref.shape[1]), BF16)
    new_ref[112:128, :] = jnp.zeros((16, HEAD), BF16)
    table_ref[0:OWN, :] = cross_ref[...]
    table_ref[128 : 128 + OWN, :] = self_ref[...]

    @pl.when((narrow & 1) == 0)
    def _():
        new_ref[0:OWN, :] = kv_ref[:, 0:HEAD]

    @pl.when((narrow & 1) == 1)
    def _():
        new_ref[0:OWN, :] = kv_ref[:, HEAD : 2 * HEAD]

    lane = lax.broadcasted_iota(jnp.int32, (64, 128), 1)
    j = lax.broadcasted_iota(jnp.int32, (64, 128), 0) & 7
    j_col = (lax.broadcasted_iota(jnp.int32, (64, 1), 0) & 7).astype(F32)
    want_extra = jnp.where(j == 6, rank, 64)
    outer_row = (outer * 8).astype(F32)
    lanes_table = iota((64, 256), 1)
    lanes_kv = iota((64, 512), 1)
    lanes_new = iota((64, 128), 1)
    for q in range(PART):
        at = 64 * q
        asked = arrived_ref[8 * q : 8 * q + 8].astype(F32)[:, 6:7, :]
        asked = jnp.broadcast_to(asked, (8, 8, 128)).reshape(64, 128)
        row = jnp.sum(jnp.where(lane == j, asked, 0.0), axis=1, keepdims=True)
        info = jnp.sum(jnp.where(lane == want_extra, asked, 0.0), axis=1, keepdims=True)
        own = jnp.where(j_col < 6.0, info * 64.0 + outer_row + j_col, -1.0)
        new = jnp.where(j_col == 6.0, info, -1.0)
        out_ref[at : at + 64, 0:768] = pick(onehot(lanes_table == row), table_ref[...]).astype(BF16)
        out_ref[at : at + 64, 768:896] = (
            pick(onehot(lanes_kv == own), arrived_ref[...].reshape(512, 128))
            + pick(onehot(lanes_new == new), new_ref[...])
        ).astype(BF16)


def unpack_kernel(arrived_ref, slot_ref, cross_ref, out_ref):
    rank = (lax.axis_index("n") >> 1).astype(F32)
    lanes = iota((128, 512), 1)
    spread = jnp.concatenate([slot_ref[0], slot_ref[1]], axis=0)[:, 0:1]
    cross_ref[...] = pick(onehot(lanes == spread), arrived_ref[:, 0:768]).astype(BF16)
    slot = jnp.concatenate(
        [slot_ref[t, 8 * k : 8 * k + 8] for k in range(PART) for t in range(2)], axis=0
    )[:, 0:1]
    self_q = pick(onehot(lanes == slot + 4.0), arrived_ref[:, 0:768]).astype(BF16)
    own_rank = slot - 8.0 * jnp.floor(slot * 0.125)
    piece = jnp.where(own_rank == rank, slot - own_rank + 6.0, -1.0)
    new = pick(onehot(lanes == piece), arrived_ref[:, 768:896]).astype(BF16)
    row = lax.broadcasted_iota(jnp.int32, (192, 512), 0)
    source = (row & 63) * 8 + (row >> 6)
    column = lax.broadcasted_iota(jnp.int32, (192, 512), 1)
    keys = pick(onehot(column == source), arrived_ref[:, 768:896]).astype(BF16)
    values = pick(onehot(column == source + 3), arrived_ref[:, 768:896]).astype(BF16)
    for k in range(PART):
        out_ref[k, :, 0:768] = self_q[16 * k : 16 * k + 16]
        out_ref[k, :, 768:896] = new[16 * k : 16 * k + 16]
        for m in range(12):
            at = 896 + 256 * m
            out_ref[k, :, at : at + 128] = keys[16 * m : 16 * m + 16]
            out_ref[k, :, at + 128 : at + 256] = values[16 * m : 16 * m + 16]


def exchange(
    enc_hidden, enc_gain, cross_weight, assign, token_ids, cross_table, self_table, kv_table
):
    tables = (cross_table, self_table, kv_table)
    asked, slot, partial, *tables = call(
        project_kernel,
        (
            pltpu.VMEM((64, 128), F32),
            pltpu.VMEM((2, 64, 128), F32),
            pltpu.VMEM((PART, 8, 896), F32),
            *[pltpu.VMEM(x.shape, x.dtype) for x in tables],
        ),
        1 << 28,
        in_specs=[vmem(), vmem(), vmem(), *[anywhere()] * 5],
        scratch_shapes=[
            pltpu.VMEM(enc_hidden.shape, BF16),
            pltpu.VMEM(cross_weight.shape, BF16),
            pltpu.SemaphoreType.DMA((5,)),
        ],
        name="project",
    )(assign, token_ids, enc_gain, enc_hidden, cross_weight, *tables)
    arrived = lax.all_to_all(partial, "n", 0, 0, tiled=True)
    finished = call(finish_kernel, pltpu.VMEM((64, 8, 128), BF16), 1 << 20, name="finish")(
        held(arrived), held(asked)
    )
    arrived = lax.all_to_all(finished, ("p", "i"), 0, 0, tiled=True)
    packed = call(
        pack_kernel,
        pltpu.VMEM((512, 896), BF16),
        1 << 28,
        scratch_shapes=[pltpu.VMEM((256, 768), BF16), pltpu.VMEM((128, 128), BF16)],
        name="pack",
    )(held(arrived), *[held(x) for x in tables])
    arrived = lax.all_to_all(packed.reshape(64, 8, 896), ("p", "i"), 0, 0, tiled=True)
    cross_q, message = call(
        unpack_kernel,
        (pltpu.VMEM((128, 768), BF16), pltpu.VMEM((PART, 16, 3968), BF16)),
        1 << 28,
        name="unpack",
    )(held(arrived.reshape(512, 896)), held(slot))
    arrived = lax.all_to_all(message, "n", 0, 0, tiled=True)
    return cross_q, arrived


def attend_kernel(
    query_ref,
    arrived_ref,
    far_cache_ref,
    cross_ref,
    self_ref,
    stack_ref,
    key_ref,
    value_ref,
    own_ref,
    result_ref,
    cache_ref,
    arrival,
):
    fetch = pltpu.make_async_copy(far_cache_ref, cache_ref, arrival)
    fetch.start()
    scale = LOG2E * HEAD ** (-0.5)
    across = (((1,), (1,)), ((), ()))

    for n in range(PART):
        for m in range(12):
            at, lane = 192 * n + 16 * m, 896 + 256 * m
            key_ref[at : at + 16, :] = arrived_ref[n, :, lane : lane + HEAD]
            value_ref[at : at + 16, :] = arrived_ref[n, :, lane + HEAD : lane + 2 * HEAD]

    for h in range(6):
        stack_ref[128 * h : 128 * h + 128, :] = query_ref[:, h * HEAD : (h + 1) * HEAD]
    def begin(b):
        query = stack_ref[256 * b : 256 * b + 256, :]
        return [
            lax.dot_general(
                query, key_ref[512 * k : 512 * k + 512, :], across, preferred_element_type=F32
            )
            for k in range(3)
        ]

    scores_ahead = begin(0)
    for b in range(3):
        scores = scores_ahead
        if b < 2:
            scores_ahead = begin(b + 1)
        peak = jnp.max(scores[0], axis=1, keepdims=True)
        for s in scores[1:]:
            peak = jnp.maximum(peak, jnp.max(s, axis=1, keepdims=True))
        total = jnp.zeros((256, 1), F32)
        result = jnp.zeros((256, HEAD), F32)
        for k in range(3):
            expo = jnp.exp2((scores[k] - peak) * scale)
            total = total + jnp.sum(expo, axis=1, keepdims=True)
            result = result + pick(expo.astype(BF16), value_ref[512 * k : 512 * k + 512, :])
        result = (result / total).astype(BF16)
        for h in range(2):
            at = (2 * b + h) * HEAD
            cross_ref[:, at : at + HEAD] = result[128 * h : 128 * h + 128]

    new_key = arrived_ref[0, :, 768:896].astype(F32)
    new_value = arrived_ref[1, :, 768:896].astype(F32)
    for n in range(2, PART, 2):
        new_key = new_key + arrived_ref[n, :, 768:896].astype(F32)
        new_value = new_value + arrived_ref[n + 1, :, 768:896].astype(F32)
    for n in range(PART):
        for h in range(6):
            tile = arrived_ref[n, :, h * HEAD : (h + 1) * HEAD].astype(F32)
            for t in range(2):
                at = 8 * (48 * t + 6 * n + h)
                own_ref[at : at + 8, :] = tile[8 * t : 8 * t + 8]

    fetch.wait()
    second = lax.broadcasted_iota(jnp.int32, (96, 1), 0) >= 48

    def start(c):
        query = own_ref[pl.ds(c, 96, stride=8), :]
        scores = lax.dot_general(
            query.astype(BF16), cache_ref[c, :, 0:HEAD], across, preferred_element_type=F32
        )
        return query, scores

    ahead = [start(0), start(1)]
    for c in range(8):
        query, scores = ahead.pop(0)
        if c < 6:
            ahead.append(start(c + 2))
        fresh = [
            jnp.sum(query * new_key[8 * j + c : 8 * j + c + 1], axis=1, keepdims=True)
            for j in range(2)
        ]
        fresh[1] = jnp.where(second, fresh[1], -jnp.inf)
        peak = jnp.max(scores, axis=1, keepdims=True)
        peak = jnp.maximum(peak, jnp.maximum(fresh[0], fresh[1]))
        expo = jnp.exp2((scores - peak) * scale)
        total = jnp.sum(expo, axis=1, keepdims=True)
        result = pick(expo.astype(BF16), cache_ref[c, :, HEAD : 2 * HEAD])
        for j in range(2):
            weight = jnp.exp2((fresh[j] - peak) * scale)
            total = total + weight
            rounded = weight.astype(BF16).astype(F32)
            result = result + rounded * new_value[8 * j + c : 8 * j + c + 1]
        result_ref[pl.ds(c, 96, stride=8), :] = result / total

    for t in range(2):
        for h in range(HEADS):
            at = 8 * (HEADS * t + h)
            self_ref[t, :, h * HEAD : (h + 1) * HEAD] = result_ref[at : at + 8, :].astype(BF16)


def attend(cross_q, arrived, self_cache):
    cross_out, self_out = call(
        attend_kernel,
        (
            jax.ShapeDtypeStruct((128, 768), BF16),
            jax.ShapeDtypeStruct((2, 8, HEADS * HEAD), BF16),
        ),
        1 << 30,
        scratch_shapes=[
            pltpu.VMEM((768, HEAD), BF16),
            pltpu.VMEM((1536, HEAD), BF16),
            pltpu.VMEM((1536, HEAD), BF16),
            pltpu.VMEM((768, HEAD), F32),
            pltpu.VMEM((768, HEAD), F32),
            pltpu.VMEM(self_cache.shape[1:], BF16),
            pltpu.SemaphoreType.DMA,
        ],
        in_specs=[vmem(), vmem(), anywhere()],
        name="attend",
    )(held(cross_q), held(arrived), self_cache[0])
    return cross_out.reshape(1, 2, 64, 768), self_out[None]


def body(*args):
    cross_q, arrived = exchange(*args[:-1])
    return attend(cross_q, arrived, args[-1])


def specs():
    wide = ("p", "i")
    ins = (
        P(wide, "n"),
        P("n"),
        P("n", None),
        P(wide),
        P(wide, None, None),
        P(wide, "n"),
        P(wide, "n"),
        P(wide, None),
        P(wide, "n", None, None),
    )
    return ins, (P(wide, None, None, "n"), P(wide, None, "n", None))


def solution(mesh):
    cut = Mesh(mesh.devices.reshape(PART, PART, PART), ("p", "i", "n"))
    ins, outs = specs()
    return jax.shard_map(body, mesh=cut, in_specs=ins, out_specs=outs, check_vma=False)
```

```python
import jax
import jax.numpy as jnp
from jax import lax
from jax.experimental import pallas as pl
from jax.experimental.pallas import tpu as pltpu
from jax.sharding import Mesh
from jax.sharding import PartitionSpec as P

D = 6144
HEADS = 48
HEAD = 128
EPS = 1e-06
OWN = 125
PART = 8
CHUNK = 24
LOG2E = 1.4426950408889634
INTERPRET = False
F32 = jnp.float32
BF16 = jnp.bfloat16


def iota(shape, dim, dtype=F32):
    return lax.broadcasted_iota(jnp.int32, shape, dim).astype(dtype)


def call(kernel, outs, flops, **kw):
    return pl.pallas_call(
        kernel,
        out_shape=outs,
        interpret=INTERPRET,
        cost_estimate=pl.CostEstimate(flops=flops, bytes_accessed=1 << 20, transcendentals=0),
        **kw,
    )


def smem():
    return pl.BlockSpec(memory_space=pltpu.SMEM)


def vmem():
    return pl.BlockSpec(memory_space=pltpu.VMEM)


def anywhere():
    return pl.BlockSpec(memory_space=pl.ANY)


def held(x):
    return pltpu.with_memory_space_constraint(x, pltpu.VMEM)


def onehot(hit):
    return jnp.where(hit, 1.0, 0.0).astype(BF16)


def pick(rows, table):
    return jnp.dot(rows, table, preferred_element_type=F32)


def request(assign_ref, ids_ref, req_ref, slot_ref):
    cand = ids_ref.shape[2]
    eye = iota((cand, cand), 0) == iota((cand, cand), 1)
    earlier = iota((cand, cand), 1) < iota((cand, cand), 0)
    lane = lax.broadcasted_iota(jnp.int32, (cand, 128), 1)
    lane_rank = jnp.where(lane < 8, lane & 3, 8).astype(F32)

    def column(row):
        return jnp.sum(jnp.where(eye, row, 0.0), axis=1, keepdims=True)

    total = jnp.zeros((64, 128), F32)
    own_rows = []
    for t in range(2):
        row = ids_ref[0, t : t + 1, :].astype(F32)
        own_row = jnp.floor((row + 0.5) * (1.0 / OWN))
        own = column(own_row)
        local = column(row) - own * OWN
        rank = jnp.sum(jnp.where(earlier & (own == own_row), 1.0, 0.0), axis=1, keepdims=True)
        for before in own_rows:
            rank = rank + jnp.sum(jnp.where(own == before, 1.0, 0.0), axis=1, keepdims=True)
        own_rows.append(own_row)
        slot_ref[t] = jnp.broadcast_to(own * 8.0 + rank, (cand, 128))
        left = onehot(iota((64, cand), 0) == own_row)
        right = jnp.where(rank == lane_rank, local + 1.0, 0.0)
        total = total + pick(left, right.astype(BF16))
    lane8 = lax.broadcasted_iota(jnp.int32, (64, 128), 1)
    asked = total - 1.0 + jnp.where((lane8 & 4) != 0, 128.0, 0.0)
    asked = jnp.where(total > 0.5, asked, -1.0)
    req_ref[...] = jnp.where(lane8 >= 64, assign_ref[0].astype(F32), asked)


def project_kernel(*refs):
    far, (req_ref, slot_ref, out_ref), near = refs[1:8], refs[8:11], (*refs[14:18], *refs[11:14])
    assign_ref, arrivals = refs[0], refs[18]
    hidden_ref, weight_ref, gain_ref, ids_ref = near[0:4]
    copies = [pltpu.make_async_copy(far[k], near[k], arrivals.at[k]) for k in range(7)]
    for copy in copies:
        copy.start()
    copies[0].wait()
    copies[2].wait()
    hidden = hidden_ref[...].astype(F32)
    scaled = (hidden * gain_ref[...].reshape(1, -1)).astype(BF16)
    copies[1].wait()
    proj = jnp.dot(scaled, weight_ref[...], preferred_element_type=F32)
    squares = jnp.sum(hidden * hidden, axis=1, keepdims=True)
    lane = lax.broadcasted_iota(jnp.int32, (8, 128), 1)
    for k in range(PART):
        tile = jnp.zeros((8, 128), F32)
        for m in range(CHUNK // 8):
            at = k * CHUNK + 8 * m
            out_ref[k, :, 256 * m : 256 * m + 256] = proj[at : at + 8]
            tile = jnp.where(lane == m, squares[at : at + 8], tile)
        out_ref[k, :, 768:896] = tile
    copies[3].wait()
    request(assign_ref, ids_ref, req_ref, slot_ref)
    for copy in copies[4:]:
        copy.wait()


def finish_kernel(arrived_ref, req_ref, out_ref):
    message = arrived_ref[0]
    for n in range(1, PART):
        message = message + arrived_ref[n]
    lane = lax.broadcasted_iota(jnp.int32, (8, 128), 1)
    row = lax.broadcasted_iota(jnp.int32, (8, 128), 0)
    parts = []
    for m in range(CHUNK // 8):
        total = jnp.sum(jnp.where(lane == m, message[:, 768:896], 0.0), axis=1, keepdims=True)
        parts.append(message[:, 256 * m : 256 * m + 256] * lax.rsqrt(total / D + EPS))
    whole = jnp.concatenate(parts, axis=0)
    for i in range(PART):
        three = whole[3 * i : 3 * i + 3]
        base = jnp.concatenate(
            [three[:, 0:HEAD], three[:, HEAD : 2 * HEAD], jnp.zeros((2, HEAD), F32)], axis=0
        )
        for p in range(PART):
            w = p * PART + i
            out_ref[w] = jnp.where(row == 6, req_ref[w : w + 1, :], base).astype(BF16)


def pack_kernel(
    arrived_ref, cross_ref, self_ref, kv_ref, out_ref, table_ref, new_ref, rows_ref
):
    outer = lax.axis_index("p")
    narrow = lax.axis_index("n")
    rank = narrow >> 1
    table_ref[112:128, :] = jnp.zeros((16, table_ref.shape[1]), BF16)
    table_ref[240:256, :] = jnp.zeros((16, table_ref.shape[1]), BF16)
    new_ref[112:128, :] = jnp.zeros((16, HEAD), BF16)
    table_ref[0:OWN, :] = cross_ref[...]
    table_ref[128 : 128 + OWN, :] = self_ref[...]

    @pl.when((narrow & 1) == 0)
    def _():
        new_ref[0:OWN, :] = kv_ref[:, 0:HEAD]

    @pl.when((narrow & 1) == 1)
    def _():
        new_ref[0:OWN, :] = kv_ref[:, HEAD : 2 * HEAD]

    lane = lax.broadcasted_iota(jnp.int32, (64, 128), 1)
    j = lax.broadcasted_iota(jnp.int32, (64, 128), 0) & 7
    j_col = (lax.broadcasted_iota(jnp.int32, (64, 1), 0) & 7).astype(F32)
    want_extra = jnp.where(j == 6, rank, 64)
    outer_row = (outer * 8).astype(F32)
    lanes_table = iota((64, 256), 1)
    lanes_kv = iota((64, 512), 1)
    lanes_new = iota((64, 128), 1)
    for q in range(PART):
        at = 64 * q
        asked = arrived_ref[8 * q : 8 * q + 8].astype(F32)[:, 6:7, :]
        asked = jnp.broadcast_to(asked, (8, 8, 128)).reshape(64, 128)
        row = jnp.sum(jnp.where(lane == j, asked, 0.0), axis=1, keepdims=True)
        info = jnp.sum(jnp.where(lane == want_extra, asked, 0.0), axis=1, keepdims=True)
        own = jnp.where(j_col < 6.0, info * 64.0 + outer_row + j_col, -1.0)
        new = jnp.where(j_col == 6.0, info, -1.0)
        rows_ref[at : at + 64, 0:256] = onehot(lanes_table == row)
        rows_ref[at : at + 64, 256:768] = onehot(lanes_kv == own)
        rows_ref[at : at + 64, 768:896] = onehot(lanes_new == new)
    for half in range(2):
        at = 256 * half
        out_ref[at : at + 256, 0:768] = pick(
            rows_ref[at : at + 256, 0:256], table_ref[...]
        ).astype(BF16)
        out_ref[at : at + 256, 768:896] = (
            pick(rows_ref[at : at + 256, 256:768], arrived_ref[...].reshape(512, 128))
            + pick(rows_ref[at : at + 256, 768:896], new_ref[...])
        ).astype(BF16)


def unpack_kernel(arrived_ref, slot_ref, cross_ref, out_ref):
    rank = (lax.axis_index("n") >> 1).astype(F32)
    lanes = iota((128, 512), 1)
    spread = jnp.concatenate([slot_ref[0], slot_ref[1]], axis=0)[:, 0:1]
    cross_ref[...] = pick(onehot(lanes == spread), arrived_ref[:, 0:768]).astype(BF16)
    slot = jnp.concatenate(
        [slot_ref[t, 8 * k : 8 * k + 8] for k in range(PART) for t in range(2)], axis=0
    )[:, 0:1]
    self_q = pick(onehot(lanes == slot + 4.0), arrived_ref[:, 0:768]).astype(BF16)
    own_rank = slot - 8.0 * jnp.floor(slot * 0.125)
    piece = jnp.where(own_rank == rank, slot - own_rank + 6.0, -1.0)
    new = pick(onehot(lanes == piece), arrived_ref[:, 768:896]).astype(BF16)
    row = lax.broadcasted_iota(jnp.int32, (192, 512), 0)
    source = (row & 63) * 8 + (row >> 6)
    column = lax.broadcasted_iota(jnp.int32, (192, 512), 1)
    keys = pick(onehot(column == source), arrived_ref[:, 768:896]).astype(BF16)
    values = pick(onehot(column == source + 3), arrived_ref[:, 768:896]).astype(BF16)
    for k in range(PART):
        out_ref[k, :, 0:768] = self_q[16 * k : 16 * k + 16]
        out_ref[k, :, 768:896] = new[16 * k : 16 * k + 16]
        for m in range(12):
            at = 896 + 256 * m
            out_ref[k, :, at : at + 128] = keys[16 * m : 16 * m + 16]
            out_ref[k, :, at + 128 : at + 256] = values[16 * m : 16 * m + 16]


def exchange(
    enc_hidden, enc_gain, cross_weight, assign, token_ids, cross_table, self_table, kv_table
):
    tables = (cross_table, self_table, kv_table)
    inputs = (enc_hidden, cross_weight, enc_gain, token_ids)
    asked, slot, partial, *tables = call(
        project_kernel,
        (
            pltpu.VMEM((64, 128), F32),
            pltpu.VMEM((2, 64, 128), F32),
            pltpu.VMEM((PART, 8, 896), F32),
            *[pltpu.VMEM(x.shape, x.dtype) for x in tables],
        ),
        1 << 28,
        in_specs=[smem(), *[anywhere()] * 7],
        scratch_shapes=[
            *[pltpu.VMEM(x.shape, x.dtype) for x in inputs],
            pltpu.SemaphoreType.DMA((7,)),
        ],
        name="project",
    )(assign, *inputs, *tables)
    arrived = lax.all_to_all(partial, "n", 0, 0, tiled=True)
    finished = call(finish_kernel, pltpu.VMEM((64, 8, 128), BF16), 1 << 20, name="finish")(
        held(arrived), held(asked)
    )
    arrived = lax.all_to_all(finished, ("p", "i"), 0, 0, tiled=True)
    packed = call(
        pack_kernel,
        pltpu.VMEM((512, 896), BF16),
        1 << 28,
        scratch_shapes=[
            pltpu.VMEM((256, 768), BF16),
            pltpu.VMEM((128, 128), BF16),
            pltpu.VMEM((512, 896), BF16),
        ],
        name="pack",
    )(held(arrived), *[held(x) for x in tables])
    arrived = lax.all_to_all(packed.reshape(64, 8, 896), ("p", "i"), 0, 0, tiled=True)
    cross_q, message = call(
        unpack_kernel,
        (pltpu.VMEM((128, 768), BF16), pltpu.VMEM((PART, 16, 3968), BF16)),
        1 << 28,
        name="unpack",
    )(held(arrived.reshape(512, 896)), held(slot))
    arrived = lax.all_to_all(message, "n", 0, 0, tiled=True)
    return cross_q, arrived


def attend_kernel(
    query_ref,
    arrived_ref,
    far_cache_ref,
    cross_ref,
    self_ref,
    stack_ref,
    key_ref,
    value_ref,
    own_ref,
    result_ref,
    cache_ref,
    arrival,
):
    fetch = pltpu.make_async_copy(far_cache_ref, cache_ref, arrival)
    fetch.start()
    scale = LOG2E * HEAD ** (-0.5)
    across = (((1,), (1,)), ((), ()))

    for n in range(PART):
        for m in range(12):
            at, lane = 192 * n + 16 * m, 896 + 256 * m
            key_ref[at : at + 16, :] = arrived_ref[n, :, lane : lane + HEAD]
            value_ref[at : at + 16, :] = arrived_ref[n, :, lane + HEAD : lane + 2 * HEAD]

    for h in range(6):
        stack_ref[128 * h : 128 * h + 128, :] = query_ref[:, h * HEAD : (h + 1) * HEAD]
    def begin(b):
        query = stack_ref[256 * b : 256 * b + 256, :]
        return [
            lax.dot_general(
                query, key_ref[512 * k : 512 * k + 512, :], across, preferred_element_type=F32
            )
            for k in range(3)
        ]

    scores_ahead = begin(0)
    for b in range(3):
        scores = scores_ahead
        if b < 2:
            scores_ahead = begin(b + 1)
        peak = jnp.max(scores[0], axis=1, keepdims=True)
        for s in scores[1:]:
            peak = jnp.maximum(peak, jnp.max(s, axis=1, keepdims=True))
        total = jnp.zeros((256, 1), F32)
        result = jnp.zeros((256, HEAD), F32)
        for k in range(3):
            expo = jnp.exp2((scores[k] - peak) * scale)
            total = total + jnp.sum(expo, axis=1, keepdims=True)
            result = result + pick(expo.astype(BF16), value_ref[512 * k : 512 * k + 512, :])
        result = (result / total).astype(BF16)
        for h in range(2):
            at = (2 * b + h) * HEAD
            cross_ref[:, at : at + HEAD] = result[128 * h : 128 * h + 128]

    new_key = arrived_ref[0, :, 768:896].astype(F32)
    new_value = arrived_ref[1, :, 768:896].astype(F32)
    for n in range(2, PART, 2):
        new_key = new_key + arrived_ref[n, :, 768:896].astype(F32)
        new_value = new_value + arrived_ref[n + 1, :, 768:896].astype(F32)
    for n in range(PART):
        for h in range(6):
            tile = arrived_ref[n, :, h * HEAD : (h + 1) * HEAD].astype(F32)
            for t in range(2):
                at = 8 * (48 * t + 6 * n + h)
                own_ref[at : at + 8, :] = tile[8 * t : 8 * t + 8]

    fetch.wait()
    second = lax.broadcasted_iota(jnp.int32, (96, 1), 0) >= 48

    def start(c):
        query = own_ref[pl.ds(c, 96, stride=8), :]
        scores = lax.dot_general(
            query.astype(BF16), cache_ref[c, :, 0:HEAD], across, preferred_element_type=F32
        )
        return query, scores

    ahead = [start(0), start(1)]
    for c in range(8):
        query, scores = ahead.pop(0)
        if c < 6:
            ahead.append(start(c + 2))
        fresh = [
            jnp.sum(query * new_key[8 * j + c : 8 * j + c + 1], axis=1, keepdims=True)
            for j in range(2)
        ]
        fresh[1] = jnp.where(second, fresh[1], -jnp.inf)
        peak = jnp.max(scores, axis=1, keepdims=True)
        peak = jnp.maximum(peak, jnp.maximum(fresh[0], fresh[1]))
        expo = jnp.exp2((scores - peak) * scale)
        total = jnp.sum(expo, axis=1, keepdims=True)
        result = pick(expo.astype(BF16), cache_ref[c, :, HEAD : 2 * HEAD])
        for j in range(2):
            weight = jnp.exp2((fresh[j] - peak) * scale)
            total = total + weight
            rounded = weight.astype(BF16).astype(F32)
            result = result + rounded * new_value[8 * j + c : 8 * j + c + 1]
        result_ref[pl.ds(c, 96, stride=8), :] = result / total

    for t in range(2):
        for h in range(HEADS):
            at = 8 * (HEADS * t + h)
            self_ref[t, :, h * HEAD : (h + 1) * HEAD] = result_ref[at : at + 8, :].astype(BF16)


def attend(cross_q, arrived, self_cache):
    cross_out, self_out = call(
        attend_kernel,
        (
            jax.ShapeDtypeStruct((128, 768), BF16),
            jax.ShapeDtypeStruct((2, 8, HEADS * HEAD), BF16),
        ),
        1 << 30,
        scratch_shapes=[
            pltpu.VMEM((768, HEAD), BF16),
            pltpu.VMEM((1536, HEAD), BF16),
            pltpu.VMEM((1536, HEAD), BF16),
            pltpu.VMEM((768, HEAD), F32),
            pltpu.VMEM((768, HEAD), F32),
            pltpu.VMEM(self_cache.shape[1:], BF16),
            pltpu.SemaphoreType.DMA,
        ],
        in_specs=[vmem(), vmem(), anywhere()],
        name="attend",
    )(held(cross_q), held(arrived), self_cache[0])
    return cross_out.reshape(1, 2, 64, 768), self_out[None]


def body(*args):
    cross_q, arrived = exchange(*args[:-1])
    return attend(cross_q, arrived, args[-1])


def specs():
    wide = ("p", "i")
    ins = (
        P(wide, "n"),
        P("n"),
        P("n", None),
        P(wide),
        P(wide, None, None),
        P(wide, "n"),
        P(wide, "n"),
        P(wide, None),
        P(wide, "n", None, None),
    )
    return ins, (P(wide, None, None, "n"), P(wide, None, "n", None))


def solution(mesh):
    cut = Mesh(mesh.devices.reshape(PART, PART, PART), ("p", "i", "n"))
    ins, outs = specs()
    return jax.shard_map(body, mesh=cut, in_specs=ins, out_specs=outs, check_vma=False)
```

```python
import jax
import jax.numpy as jnp
from jax import lax
from jax.experimental import pallas as pl
from jax.experimental.pallas import tpu as pltpu
from jax.sharding import Mesh
from jax.sharding import PartitionSpec as P

D = 6144
HEADS = 48
HEAD = 128
EPS = 1e-06
OWN = 125
PART = 8
CHUNK = 24
LOG2E = 1.4426950408889634
INTERPRET = False
F32 = jnp.float32
BF16 = jnp.bfloat16


def iota(shape, dim, dtype=F32):
    return lax.broadcasted_iota(jnp.int32, shape, dim).astype(dtype)


def call(kernel, outs, flops, **kw):
    return pl.pallas_call(
        kernel,
        out_shape=outs,
        interpret=INTERPRET,
        cost_estimate=pl.CostEstimate(flops=flops, bytes_accessed=1 << 20, transcendentals=0),
        **kw,
    )


def smem():
    return pl.BlockSpec(memory_space=pltpu.SMEM)


def vmem():
    return pl.BlockSpec(memory_space=pltpu.VMEM)


def anywhere():
    return pl.BlockSpec(memory_space=pl.ANY)


def held(x):
    return pltpu.with_memory_space_constraint(x, pltpu.VMEM)


def onehot(hit):
    return jnp.where(hit, 1.0, 0.0).astype(BF16)


def pick(rows, table):
    return jnp.dot(rows, table, preferred_element_type=F32)


def request(assign_ref, ids_ref, req_ref, slot_ref):
    cand = ids_ref.shape[2]
    eye = iota((cand, cand), 0) == iota((cand, cand), 1)
    earlier = iota((cand, cand), 1) < iota((cand, cand), 0)
    lane = lax.broadcasted_iota(jnp.int32, (cand, 128), 1)
    lane_rank = jnp.where(lane < 8, lane & 3, 8).astype(F32)

    def column(row):
        return jnp.sum(jnp.where(eye, row, 0.0), axis=1, keepdims=True)

    total = jnp.zeros((64, 128), F32)
    own_rows = []
    for t in range(2):
        row = ids_ref[0, t : t + 1, :].astype(F32)
        own_row = jnp.floor((row + 0.5) * (1.0 / OWN))
        own = column(own_row)
        local = column(row) - own * OWN
        rank = jnp.sum(jnp.where(earlier & (own == own_row), 1.0, 0.0), axis=1, keepdims=True)
        for before in own_rows:
            rank = rank + jnp.sum(jnp.where(own == before, 1.0, 0.0), axis=1, keepdims=True)
        own_rows.append(own_row)
        slot_ref[t] = jnp.broadcast_to(own * 8.0 + rank, (cand, 128))
        left = onehot(iota((64, cand), 0) == own_row)
        right = jnp.where(rank == lane_rank, local + 1.0, 0.0)
        total = total + pick(left, right.astype(BF16))
    lane8 = lax.broadcasted_iota(jnp.int32, (64, 128), 1)
    asked = total - 1.0 + jnp.where((lane8 & 4) != 0, 128.0, 0.0)
    asked = jnp.where(total > 0.5, asked, -1.0)
    req_ref[...] = jnp.where(lane8 >= 64, assign_ref[0].astype(F32), asked)


def project_kernel(*refs):
    far, (req_ref, slot_ref, out_ref), near = refs[1:8], refs[8:11], (*refs[14:18], *refs[11:14])
    assign_ref, arrivals = refs[0], refs[18]
    hidden_ref, weight_ref, gain_ref, ids_ref = near[0:4]
    copies = [pltpu.make_async_copy(far[k], near[k], arrivals.at[k]) for k in range(7)]
    for copy in copies:
        copy.start()
    copies[0].wait()
    copies[2].wait()
    hidden = hidden_ref[...].astype(F32)
    scaled = (hidden * gain_ref[...].reshape(1, -1)).astype(BF16)
    copies[1].wait()
    proj = jnp.dot(scaled, weight_ref[...], preferred_element_type=F32)
    squares = jnp.sum(hidden * hidden, axis=1, keepdims=True)
    lane = lax.broadcasted_iota(jnp.int32, (8, 128), 1)
    for k in range(PART):
        tile = jnp.zeros((8, 128), F32)
        for m in range(CHUNK // 8):
            at = k * CHUNK + 8 * m
            out_ref[k, :, 256 * m : 256 * m + 256] = proj[at : at + 8]
            tile = jnp.where(lane == m, squares[at : at + 8], tile)
        out_ref[k, :, 768:896] = tile
    copies[3].wait()
    request(assign_ref, ids_ref, req_ref, slot_ref)
    for copy in copies[4:]:
        copy.wait()


def finish_kernel(arrived_ref, req_ref, out_ref):
    message = arrived_ref[0]
    for n in range(1, PART):
        message = message + arrived_ref[n]
    lane = lax.broadcasted_iota(jnp.int32, (8, 128), 1)
    row = lax.broadcasted_iota(jnp.int32, (8, 128), 0)
    parts = []
    for m in range(CHUNK // 8):
        total = jnp.sum(jnp.where(lane == m, message[:, 768:896], 0.0), axis=1, keepdims=True)
        parts.append(message[:, 256 * m : 256 * m + 256] * lax.rsqrt(total / D + EPS))
    whole = jnp.concatenate(parts, axis=0)
    for i in range(PART):
        three = whole[3 * i : 3 * i + 3]
        base = jnp.concatenate(
            [three[:, 0:HEAD], three[:, HEAD : 2 * HEAD], jnp.zeros((2, HEAD), F32)], axis=0
        )
        for p in range(PART):
            w = p * PART + i
            out_ref[w] = jnp.where(row == 6, req_ref[w : w + 1, :], base).astype(BF16)


def pack_kernel(
    arrived_ref, cross_ref, self_ref, kv_ref, out_ref, table_ref, new_ref, rows_ref
):
    outer = lax.axis_index("p")
    narrow = lax.axis_index("n")
    rank = narrow >> 1
    table_ref[112:128, :] = jnp.zeros((16, table_ref.shape[1]), BF16)
    table_ref[240:256, :] = jnp.zeros((16, table_ref.shape[1]), BF16)
    new_ref[112:128, :] = jnp.zeros((16, HEAD), BF16)
    table_ref[0:OWN, :] = cross_ref[...]
    table_ref[128 : 128 + OWN, :] = self_ref[...]

    @pl.when((narrow & 1) == 0)
    def _():
        new_ref[0:OWN, :] = kv_ref[:, 0:HEAD]

    @pl.when((narrow & 1) == 1)
    def _():
        new_ref[0:OWN, :] = kv_ref[:, HEAD : 2 * HEAD]

    lane = lax.broadcasted_iota(jnp.int32, (64, 128), 1)
    j = lax.broadcasted_iota(jnp.int32, (64, 128), 0) & 7
    j_col = (lax.broadcasted_iota(jnp.int32, (64, 1), 0) & 7).astype(F32)
    want_extra = jnp.where(j == 6, rank, 64)
    outer_row = (outer * 8).astype(F32)
    lanes_table = iota((64, 256), 1)
    lanes_kv = iota((64, 512), 1)
    lanes_new = iota((64, 128), 1)
    for q in range(PART):
        at = 64 * q
        asked = arrived_ref[8 * q : 8 * q + 8].astype(F32)[:, 6:7, :]
        asked = jnp.broadcast_to(asked, (8, 8, 128)).reshape(64, 128)
        row = jnp.sum(jnp.where(lane == j, asked, 0.0), axis=1, keepdims=True)
        info = jnp.sum(jnp.where(lane == want_extra, asked, 0.0), axis=1, keepdims=True)
        own = jnp.where(j_col < 6.0, info * 64.0 + outer_row + j_col, -1.0)
        new = jnp.where(j_col == 6.0, info, -1.0)
        rows_ref[at : at + 64, 0:256] = onehot(lanes_table == row)
        rows_ref[at : at + 64, 256:768] = onehot(lanes_kv == own)
        rows_ref[at : at + 64, 768:896] = onehot(lanes_new == new)
    for half in range(2):
        at = 256 * half
        out_ref[at : at + 256, 0:768] = pick(
            rows_ref[at : at + 256, 0:256], table_ref[...]
        ).astype(BF16)
        out_ref[at : at + 256, 768:896] = (
            pick(rows_ref[at : at + 256, 256:768], arrived_ref[...].reshape(512, 128))
            + pick(rows_ref[at : at + 256, 768:896], new_ref[...])
        ).astype(BF16)


def unpack_kernel(arrived_ref, slot_ref, cross_ref, out_ref):
    rank = (lax.axis_index("n") >> 1).astype(F32)
    lanes = iota((128, 512), 1)
    spread = jnp.concatenate([slot_ref[0], slot_ref[1]], axis=0)[:, 0:1]
    slot = jnp.concatenate(
        [slot_ref[t, 8 * k : 8 * k + 8] for k in range(PART) for t in range(2)], axis=0
    )[:, 0:1]
    queries = pick(
        jnp.concatenate([onehot(lanes == spread), onehot(lanes == slot + 4.0)], axis=0),
        arrived_ref[:, 0:768],
    ).astype(BF16)
    cross_ref[...] = queries[0:128]
    self_q = queries[128:256]
    own_rank = slot - 8.0 * jnp.floor(slot * 0.125)
    piece = jnp.where(own_rank == rank, slot - own_rank + 6.0, -1.0)
    row = lax.broadcasted_iota(jnp.int32, (192, 512), 0)
    source = (row & 63) * 8 + (row >> 6)
    column = lax.broadcasted_iota(jnp.int32, (192, 512), 1)
    beside = pick(
        jnp.concatenate(
            [onehot(lanes == piece), onehot(column == source), onehot(column == source + 3)], axis=0
        ),
        arrived_ref[:, 768:896],
    ).astype(BF16)
    new, keys, values = beside[0:128], beside[128:320], beside[320:512]
    for k in range(PART):
        out_ref[k, :, 0:768] = self_q[16 * k : 16 * k + 16]
        out_ref[k, :, 768:896] = new[16 * k : 16 * k + 16]
        for m in range(12):
            at = 896 + 256 * m
            out_ref[k, :, at : at + 128] = keys[16 * m : 16 * m + 16]
            out_ref[k, :, at + 128 : at + 256] = values[16 * m : 16 * m + 16]


def exchange(
    enc_hidden, enc_gain, cross_weight, assign, token_ids, cross_table, self_table, kv_table
):
    tables = (cross_table, self_table, kv_table)
    inputs = (enc_hidden, cross_weight, enc_gain, token_ids)
    asked, slot, partial, *tables = call(
        project_kernel,
        (
            pltpu.VMEM((64, 128), F32),
            pltpu.VMEM((2, 64, 128), F32),
            pltpu.VMEM((PART, 8, 896), F32),
            *[pltpu.VMEM(x.shape, x.dtype) for x in tables],
        ),
        1 << 28,
        in_specs=[smem(), *[anywhere()] * 7],
        scratch_shapes=[
            *[pltpu.VMEM(x.shape, x.dtype) for x in inputs],
            pltpu.SemaphoreType.DMA((7,)),
        ],
        name="project",
    )(assign, *inputs, *tables)
    arrived = lax.all_to_all(partial, "n", 0, 0, tiled=True)
    finished = call(finish_kernel, pltpu.VMEM((64, 8, 128), BF16), 1 << 20, name="finish")(
        held(arrived), held(asked)
    )
    arrived = lax.all_to_all(finished, ("p", "i"), 0, 0, tiled=True)
    packed = call(
        pack_kernel,
        pltpu.VMEM((512, 896), BF16),
        1 << 28,
        scratch_shapes=[
            pltpu.VMEM((256, 768), BF16),
            pltpu.VMEM((128, 128), BF16),
            pltpu.VMEM((512, 896), BF16),
        ],
        name="pack",
    )(held(arrived), *[held(x) for x in tables])
    arrived = lax.all_to_all(packed.reshape(64, 8, 896), ("p", "i"), 0, 0, tiled=True)
    cross_q, message = call(
        unpack_kernel,
        (pltpu.VMEM((128, 768), BF16), pltpu.VMEM((PART, 16, 3968), BF16)),
        1 << 28,
        name="unpack",
    )(held(arrived.reshape(512, 896)), held(slot))
    arrived = lax.all_to_all(message, "n", 0, 0, tiled=True)
    return cross_q, arrived


def attend_kernel(
    query_ref,
    arrived_ref,
    far_cache_ref,
    cross_ref,
    self_ref,
    stack_ref,
    key_ref,
    value_ref,
    own_ref,
    result_ref,
    cache_ref,
    arrival,
):
    fetch = pltpu.make_async_copy(far_cache_ref, cache_ref, arrival)
    fetch.start()
    scale = LOG2E * HEAD ** (-0.5)
    across = (((1,), (1,)), ((), ()))

    for n in range(PART):
        for m in range(12):
            at, lane = 192 * n + 16 * m, 896 + 256 * m
            key_ref[at : at + 16, :] = arrived_ref[n, :, lane : lane + HEAD]
            value_ref[at : at + 16, :] = arrived_ref[n, :, lane + HEAD : lane + 2 * HEAD]

    for h in range(6):
        stack_ref[128 * h : 128 * h + 128, :] = query_ref[:, h * HEAD : (h + 1) * HEAD]
    def begin(b):
        query = stack_ref[256 * b : 256 * b + 256, :]
        return [
            lax.dot_general(
                query, key_ref[512 * k : 512 * k + 512, :], across, preferred_element_type=F32
            )
            for k in range(3)
        ]

    scores_ahead = begin(0)
    for b in range(3):
        scores = scores_ahead
        if b < 2:
            scores_ahead = begin(b + 1)
        peak = jnp.max(scores[0], axis=1, keepdims=True)
        for s in scores[1:]:
            peak = jnp.maximum(peak, jnp.max(s, axis=1, keepdims=True))
        total = jnp.zeros((256, 1), F32)
        result = jnp.zeros((256, HEAD), F32)
        for k in range(3):
            expo = jnp.exp2((scores[k] - peak) * scale)
            total = total + jnp.sum(expo, axis=1, keepdims=True)
            result = result + pick(expo.astype(BF16), value_ref[512 * k : 512 * k + 512, :])
        result = (result / total).astype(BF16)
        for h in range(2):
            at = (2 * b + h) * HEAD
            cross_ref[:, at : at + HEAD] = result[128 * h : 128 * h + 128]

    new_key = arrived_ref[0, :, 768:896].astype(F32)
    new_value = arrived_ref[1, :, 768:896].astype(F32)
    for n in range(2, PART, 2):
        new_key = new_key + arrived_ref[n, :, 768:896].astype(F32)
        new_value = new_value + arrived_ref[n + 1, :, 768:896].astype(F32)
    for n in range(PART):
        for h in range(6):
            tile = arrived_ref[n, :, h * HEAD : (h + 1) * HEAD].astype(F32)
            for t in range(2):
                at = 8 * (48 * t + 6 * n + h)
                own_ref[at : at + 8, :] = tile[8 * t : 8 * t + 8]

    fetch.wait()
    second = lax.broadcasted_iota(jnp.int32, (96, 1), 0) >= 48

    def start(c):
        query = own_ref[pl.ds(c, 96, stride=8), :]
        scores = lax.dot_general(
            query.astype(BF16), cache_ref[c, :, 0:HEAD], across, preferred_element_type=F32
        )
        return query, scores

    ahead = [start(0), start(1)]
    for c in range(8):
        query, scores = ahead.pop(0)
        if c < 6:
            ahead.append(start(c + 2))
        fresh = [
            jnp.sum(query * new_key[8 * j + c : 8 * j + c + 1], axis=1, keepdims=True)
            for j in range(2)
        ]
        fresh[1] = jnp.where(second, fresh[1], -jnp.inf)
        peak = jnp.max(scores, axis=1, keepdims=True)
        peak = jnp.maximum(peak, jnp.maximum(fresh[0], fresh[1]))
        expo = jnp.exp2((scores - peak) * scale)
        total = jnp.sum(expo, axis=1, keepdims=True)
        result = pick(expo.astype(BF16), cache_ref[c, :, HEAD : 2 * HEAD])
        for j in range(2):
            weight = jnp.exp2((fresh[j] - peak) * scale)
            total = total + weight
            rounded = weight.astype(BF16).astype(F32)
            result = result + rounded * new_value[8 * j + c : 8 * j + c + 1]
        result_ref[pl.ds(c, 96, stride=8), :] = result / total

    for t in range(2):
        for h in range(HEADS):
            at = 8 * (HEADS * t + h)
            self_ref[t, :, h * HEAD : (h + 1) * HEAD] = result_ref[at : at + 8, :].astype(BF16)


def attend(cross_q, arrived, self_cache):
    cross_out, self_out = call(
        attend_kernel,
        (
            jax.ShapeDtypeStruct((128, 768), BF16),
            jax.ShapeDtypeStruct((2, 8, HEADS * HEAD), BF16),
        ),
        1 << 30,
        scratch_shapes=[
            pltpu.VMEM((768, HEAD), BF16),
            pltpu.VMEM((1536, HEAD), BF16),
            pltpu.VMEM((1536, HEAD), BF16),
            pltpu.VMEM((768, HEAD), F32),
            pltpu.VMEM((768, HEAD), F32),
            pltpu.VMEM(self_cache.shape[1:], BF16),
            pltpu.SemaphoreType.DMA,
        ],
        in_specs=[vmem(), vmem(), anywhere()],
        name="attend",
    )(held(cross_q), held(arrived), self_cache[0])
    return cross_out.reshape(1, 2, 64, 768), self_out[None]


def body(*args):
    cross_q, arrived = exchange(*args[:-1])
    return attend(cross_q, arrived, args[-1])


def specs():
    wide = ("p", "i")
    ins = (
        P(wide, "n"),
        P("n"),
        P("n", None),
        P(wide),
        P(wide, None, None),
        P(wide, "n"),
        P(wide, "n"),
        P(wide, None),
        P(wide, "n", None, None),
    )
    return ins, (P(wide, None, None, "n"), P(wide, None, "n", None))


def solution(mesh):
    cut = Mesh(mesh.devices.reshape(PART, PART, PART), ("p", "i", "n"))
    ins, outs = specs()
    return jax.shard_map(body, mesh=cut, in_specs=ins, out_specs=outs, check_vma=False)
```
